32 devices in a mesh: gx: 4 (over x, core), gy: 8 (over z, y).
Axes of the slice: x: 2, y: 2, z: 4, core: 2. Of those that a mesh axis runs over, the one named last changes fastest.
Arguments:
- emission: bfloat16 [98304, 128], P(('gx', 'gy')), may hold values from -6 to 6
- reflectance: float32 [98304], P(('gx', 'gy')), may hold values from 0.3 to 0.9
- link_blocks: bfloat16 [4608, 256, 256], P(('gx', 'gy')), may hold values from -0.109375 to 0.109375
- link_source: int32 [4608], P(('gx', 'gy')), may hold values from 0 to 11
- link_target: int32 [4608, 1], P(('gx', 'gy')), may hold values from 0 to 31, as said below
- link_slot: int32 [4608], P(('gx', 'gy')), may hold values from 0 to 11
- sensor_cell: int32 [16384, 8], P(('gx', 'gy')), may hold values from 0 to 9215
- sensor_weight: float32 [16384, 8], P(('gx', 'gy')), may hold values from 0 to 0.25
Outputs:
- radiosity: float32 [98304, 128], P(('gx', 'gy'))
- sensor_values: float32 [16384, 128], P(('gx', 'gy'))
The draws below stay inside these ranges and needn't reach their ends.
Inputs may be any that keep to these rules, and one draw needn't show every extreme that they name: `link_target`: the owner of each block is the device that holds it or one of that device's neighbours (i +- 1, j) or (i, j +- 1) inside the grid of devices, without wrapping. Among the 144 blocks of one device at most 9 name any one neighbour, and some neighbour is named exactly 9 times.
All inputs are finite; a program needn't handle non-finite values.
Results may differ from the reference program's by a relative error of at most 0.0039.
Values may be sent and summed in bfloat16 or wider, within the bound.
A program may use at most 128 MiB of HBM per device.

```python
import jax
import jax.numpy as jnp
from jax import lax

P_SIZE = 256
S = 128
CL_DEV = 12
LINKS = 12
SWEEPS = 2
SENS_DEV = 512
TAPS = 8
CLUSTERS = 384
LINK_DEV = 144
LINKS_ALL = 4608
CAP = 9
SENSORS = 16384
N_GX = 4
N_GY = 8


def draw_link_target(key, part):
    devices = N_GX * N_GY
    index = jnp.arange(devices, dtype=jnp.int32)
    row = index // N_GY
    col = index % N_GY
    exists = jnp.stack([row + 1 < N_GX, row >= 1, col + 1 < N_GY, col >= 1], axis=1).astype(jnp.int32)
    owners = jnp.stack([index + N_GY, index - N_GY, index + 1, index - 1, index], axis=1)
    first_key, second_key, third_key = jax.random.split(jax.random.fold_in(key, 11), 3)
    lowest = max(1, CAP // 2)
    counts = jax.random.randint(first_key, (devices, 4), lowest, CAP + 1).astype(jnp.int32) * exists
    start = jax.random.randint(second_key, (devices,), 0, 4).astype(jnp.int32)
    order = (start[:, None] + jnp.arange(4, dtype=jnp.int32)[None, :]) % 4
    exists_turned = jnp.take_along_axis(exists, order, axis=1)
    first = jnp.argmax(exists_turned, axis=1).astype(jnp.int32)
    picked = jnp.take_along_axis(order, first[:, None], axis=1)[:, 0]
    counts = jnp.where(jnp.arange(4, dtype=jnp.int32)[None, :] == picked[:, None], CAP, counts)
    edges = jnp.cumsum(counts, axis=1)
    position = jnp.arange(LINK_DEV, dtype=jnp.int32)
    label = jnp.sum((position[None, :, None] >= edges[:, None, :]).astype(jnp.int32), axis=2)
    target = jnp.take_along_axis(owners, label, axis=1)
    scores = jax.random.randint(third_key, (devices, LINK_DEV), 0, 1 << 20).astype(jnp.int32) * LINK_DEV + position[None, :]
    shuffle = jnp.argsort(scores, axis=1)
    target = jnp.take_along_axis(target, shuffle, axis=1)
    return target.reshape(devices * LINK_DEV, 1).astype(jnp.int32)


def place_ends(drawn, key, smallest, high):
    longest = drawn.shape.index(max(drawn.shape))
    spots = []
    for shift in (0, 1):
        where = [jax.random.randint(jax.random.fold_in(key, axis), (), 0, length) for axis, length in enumerate(drawn.shape)]
        where[longest] = (where[longest] + shift) % drawn.shape[longest]
        spots.append(tuple(where))
    return drawn.at[spots[0]].set(smallest).at[spots[1]].set(high)


def shard_levels(key, extent, cuts, smallest, largest):
    factor_of, own = 1.0, jax.random.fold_in(key, 6)
    for dim, shards_of in cuts:
        heights = jnp.exp(jax.random.uniform(jax.random.fold_in(own, dim), (shards_of,), jnp.float32, smallest / len(cuts), largest / len(cuts)))
        factor_of = factor_of * jnp.repeat(heights, extent[dim] // shards_of).reshape([-1 if axis == dim else 1 for axis in range(len(extent))])
    return factor_of


def centred(key, dims, spread, bound, shards=(), kind=jnp.bfloat16):
    gain = shard_levels(key, dims, shards, -0.22, 0.18) if shards else 1.0
    array = jax.random.normal(key, dims, jnp.float32) * spread * gain
    return jnp.minimum(jnp.maximum(array, -bound), bound).astype(kind)


def setup_inputs(seed: int = 0) -> dict:
    arg_keys = jax.random.split(jax.random.key(seed), 9)
    emission = centred(arg_keys[0], (CLUSTERS * P_SIZE, S), 1.0, 6.0, ((0, 32),))
    reflectance = jnp.clip(0.3 + 0.59999996 * jax.random.uniform(arg_keys[1], (CLUSTERS * P_SIZE,), jnp.float32) ** shard_levels(arg_keys[1], (CLUSTERS * P_SIZE,), ((0, 32),), -0.2, 0.2), 0.3, 0.9)
    link_blocks = centred(arg_keys[2], (LINKS_ALL, P_SIZE, P_SIZE), (P_SIZE * LINKS) ** -0.5, 0.109375, ((0, 32),))
    link_source = place_ends(jax.random.randint(arg_keys[3], (LINKS_ALL,), 0, CL_DEV), jax.random.fold_in(arg_keys[3], 1), 0, CL_DEV - 1).astype(jnp.int32)
    link_target = draw_link_target(jax.random.fold_in(arg_keys[8], 71), 0)
    link_slot = place_ends(jax.random.randint(arg_keys[5], (LINKS_ALL,), 0, CL_DEV), jax.random.fold_in(arg_keys[5], 1), 0, CL_DEV - 1).astype(jnp.int32)
    sensor_cell = place_ends(jax.random.randint(arg_keys[6], (SENSORS, TAPS), 0, 3 * CL_DEV * P_SIZE), jax.random.fold_in(arg_keys[6], 1), 0, (3 * CL_DEV * P_SIZE) - 1).astype(jnp.int32)
    sensor_weight = jnp.clip(0.25 * jax.random.uniform(arg_keys[7], (SENSORS, TAPS), jnp.float32) ** shard_levels(arg_keys[7], (SENSORS, TAPS), ((0, 32),), -0.2, 0.2), 0.0, 0.25)
    return {"emission": emission, "reflectance": reflectance, "link_blocks": link_blocks, "link_source": link_source, "link_target": link_target, "link_slot": link_slot, "sensor_cell": sensor_cell, "sensor_weight": sensor_weight}


def reference(emission, reflectance, link_blocks, link_source, link_target, link_slot, sensor_cell, sensor_weight):
    devices = N_GX * N_GY
    clusters = CL_DEV * devices
    base = emission.astype(jnp.float32)
    blocks = link_blocks.reshape(devices, LINK_DEV, P_SIZE, P_SIZE)
    offsets = (CL_DEV * jnp.arange(devices, dtype=jnp.int32))[:, None]
    sources = (link_source.reshape(devices, LINK_DEV) + offsets).astype(jnp.int32)
    targets = (link_target[:, 0] * CL_DEV + link_slot).reshape(devices, LINK_DEV).astype(jnp.int32)
    radiosity = base
    for sweep in range(SWEEPS):
        rounded = radiosity.astype(jnp.bfloat16)
        rounded = lax.optimization_barrier(rounded).astype(jnp.float32).reshape(clusters, P_SIZE, S)

        def step(incoming, item):
            block, source, target = item
            term = jnp.einsum("lpq,lqs->lps", block.astype(jnp.float32), rounded[source],
                              precision=lax.Precision.HIGHEST).astype(jnp.bfloat16)
            term = lax.optimization_barrier(term).astype(jnp.float32)
            return incoming.at[target].add(term), None

        incoming, _ = lax.scan(step, jnp.zeros((clusters, P_SIZE, S), jnp.float32), (blocks, sources, targets))
        radiosity = base + reflectance[:, None] * incoming.reshape(clusters * P_SIZE, S)
    rows = CL_DEV * P_SIZE
    final = radiosity.astype(jnp.bfloat16).reshape(N_GX, N_GY, rows, S)
    padded = jnp.pad(final, ((0, 0), (1, 1), (0, 0), (0, 0))).reshape(-1, S)
    device_of = (jnp.arange(SENS_DEV * devices, dtype=jnp.int32) // SENS_DEV).astype(jnp.int32)
    row_index = (device_of // N_GY).astype(jnp.int32)
    col_index = (device_of % N_GY).astype(jnp.int32)
    which = sensor_cell // rows
    within = sensor_cell % rows
    flat = ((row_index[:, None] * (N_GY + 2) + col_index[:, None] + which) * rows + within).astype(jnp.int32)
    sensor_values = jnp.zeros((SENS_DEV * devices, S), jnp.float32)
    for tap in range(TAPS):
        sensor_values = sensor_values + sensor_weight[:, tap][:, None] * padded[flat[:, tap]].astype(jnp.float32)
    return radiosity, sensor_values
```

```python
import functools
import math

import jax
import jax.numpy as jnp
from jax import lax
from jax.experimental import pallas as pl
from jax.experimental.pallas import tpu as pltpu
from jax.sharding import PartitionSpec as P

P_SIZE = 256
S = 128
SWEEPS = 2
TAPS = 8
MOVES = (("gx", 1), ("gx", -1), ("gy", 1), ("gy", -1))


def passed_along(block, axis, distance):
    devices = range(lax.axis_size(axis))
    route = [(i - distance, i) for i in devices if i - distance in devices]
    return lax.ppermute(block, axis, route)


def per_step_of(*counts):
    common = math.gcd(*counts)
    return max(n for n in range(1, 13) if common % n == 0)


def combine_into(acc_ref, slot_ref, arrived, emission_ref, refl_ref, rounded_ref, rad_ref, capacity, clusters):
    for way in range(4):
        def add(r, carry, way=way):
            slot = slot_ref[way * capacity + r]
            rows = pl.ds(pl.multiple_of(r * P_SIZE, P_SIZE), P_SIZE)
            acc_ref[slot] += arrived[way][rows, :].astype(jnp.float32)
            return carry
        lax.fori_loop(0, capacity, add, 0)

    def finish(c, carry):
        value = emission_ref[c].astype(jnp.float32) + refl_ref[c] * acc_ref[c]
        rounded_ref[c] = value.astype(jnp.bfloat16)
        if rad_ref is not None:
            rad_ref[c] = value
        return carry
    lax.fori_loop(0, clusters, finish, 0)


def outgoing_kernel(order, source, place, slot, *refs, first, per_step, capacity, clusters, extra):
    blocks, refs = refs[:per_step], refs[per_step:]
    if first:
        emission, tail = refs[:2]
        refs = refs[2:]
        rounded = emission
    else:
        acc_in, a0, a1, a2, a3, emission, refl = refs[:7]
        rounded = refs[7]
        refs = refs[8:]
    local, sends, acc = refs[0], refs[1:5], refs[5]
    step = pl.program_id(0)

    @pl.when(step == 0)
    def _():
        if not first:
            acc[0:clusters] = acc_in[...]
            combine_into(acc, slot, (a0, a1, a2, a3), emission, refl, rounded, None, capacity, clusters)
        acc[...] = jnp.zeros(acc.shape, acc.dtype)

    for g in range(per_step):
        at = step * per_step + g
        acc[place[at]] += jnp.dot(blocks[g][...], rounded[source[at]], preferred_element_type=jnp.float32)

    @pl.when(step == pl.num_programs(0) - 1)
    def _():
        local[...] = acc[0:clusters]
        for way in range(4):
            for r in range(capacity):
                sends[way][r * P_SIZE : (r + 1) * P_SIZE, :] = acc[clusters + way * capacity + r].astype(jnp.bfloat16)
            if first:
                sends[way][capacity * P_SIZE :, :] = tail[way]


def local_kernel(order, source, place, *refs, per_step, offset):
    blocks, refs = refs[:per_step], refs[per_step:]
    rounded, acc_in, acc = refs
    step = pl.program_id(0)

    @pl.when(step == 0)
    def _():
        acc[...] = acc_in[...]

    for g in range(per_step):
        at = offset + step * per_step + g
        acc[place[at]] += jnp.dot(blocks[g][...], rounded[source[at]], preferred_element_type=jnp.float32)


def final_kernel(slot, acc_in, a0, a1, a2, a3, emission, refl, rounded, rad, acc, *, capacity, clusters):
    acc[...] = acc_in[...]
    combine_into(acc, slot, (a0, a1, a2, a3), emission, refl, rounded, rad, capacity, clusters)


def weights_kernel(item_ref, out_ref, *, tile, columns):
    def body(t, carry):
        rows = pl.ds(pl.multiple_of(t * tile, tile), tile)
        item = item_ref[rows, :]
        cells = [jnp.broadcast_to(item[:, k : k + 1], (tile, 128)) for k in range(TAPS)]
        weights = [jnp.broadcast_to(item[:, TAPS + k : TAPS + k + 1], (tile, 128)) for k in range(TAPS)]
        lane = lax.broadcasted_iota(jnp.int32, (tile, 128), 1).astype(jnp.float32)
        for c in range(columns // 128):
            here = lane + float(c * 128)
            total = jnp.where(cells[0] == here, weights[0], 0.0)
            for k in range(1, TAPS):
                total = total + jnp.where(cells[k] == here, weights[k], 0.0)
            out_ref[rows, c * 128 : (c + 1) * 128] = total.astype(jnp.bfloat16)
        return carry
    lax.fori_loop(0, item_ref.shape[0] // tile, body, 0)


def whole(shape):
    return pl.BlockSpec(shape, lambda *_: (0,) * len(shape))


def block_specs(per_step, offset):
    return [
        pl.BlockSpec((None, P_SIZE, P_SIZE), lambda i, order, *_, g=g: (order[offset + i * per_step + g], 0, 0))
        for g in range(per_step)
    ]


def per_device(
    emission,
    reflectance,
    link_blocks,
    link_source,
    link_target,
    link_slot,
    sensor_cell,
    sensor_weight,
):
    n_cols = lax.axis_size("gy")
    row_here = lax.axis_index("gx")
    col_here = lax.axis_index("gy")
    device_here = row_here * n_cols + col_here
    count_links = link_blocks.shape[0]
    rows_here = emission.shape[0]
    clusters = rows_here // P_SIZE
    capacity = max(2, count_links // 16)
    extra = -(-capacity // 16) * 16
    outgoing = 4 * capacity
    per_step = per_step_of(outgoing, count_links)
    full = (clusters, P_SIZE, S)
    send_rows = capacity * P_SIZE

    owner = link_target[:, 0]
    owner_row = owner // n_cols
    owner_col = owner % n_cols
    heading = jnp.where(
        owner == device_here,
        0,
        jnp.where(
            owner_row == row_here + 1,
            1,
            jnp.where(owner_row == row_here - 1, 2, jnp.where(owner_col == col_here + 1, 3, 4)),
        ),
    ).astype(jnp.int32)
    number = jnp.arange(count_links, dtype=jnp.int32)
    before = number[None, :] < number[:, None]
    rank = jnp.sum(((heading[:, None] == heading[None, :]) & before).astype(jnp.int32), axis=1)
    local = heading == 0
    ahead = jnp.where(local[:, None], (~local)[None, :] | before, (~local)[None, :] & before)
    position = jnp.sum(ahead.astype(jnp.int32), axis=1)
    place = jnp.where(local, link_slot, clusters + (heading - 1) * capacity + rank)
    turned = position[None, :] == number[:, None]

    def sort(x):
        return jnp.sum(jnp.where(turned, x[None, :], 0), axis=1)

    order, source, place_sorted = sort(number), sort(link_source), sort(place)
    spots = clusters + jnp.arange(outgoing, dtype=jnp.int32)
    sent_slot = jnp.sum(jnp.where(place[None, :] == spots[:, None], (link_slot * (~local))[None, :], 0), axis=1)
    tail = jnp.zeros((4, extra), jnp.bfloat16).at[:, :capacity].set(
        sent_slot.reshape(4, capacity).astype(jnp.bfloat16)
    )
    tail = jnp.broadcast_to(tail[:, :, None], (4, extra, S))

    item = jnp.concatenate([sensor_cell.astype(jnp.float32), sensor_weight], axis=1)
    item_before = passed_along(item, "gy", 1)
    item_after = passed_along(item, "gy", -1)

    emission3 = emission.reshape(full)
    refl = jnp.broadcast_to(reflectance[:, None], (rows_here, S)).reshape(full)
    params = pltpu.CompilerParams(dimension_semantics=("arbitrary",), vmem_limit_bytes=56 * 2**20)

    def leave(first, slot, *state):
        rows = send_rows + (extra if first else 0)
        out_shape = [jax.ShapeDtypeStruct(full, jnp.float32)] + [jax.ShapeDtypeStruct((rows, S), jnp.bfloat16)] * 4
        if not first:
            out_shape = [jax.ShapeDtypeStruct(full, jnp.bfloat16)] + out_shape
        return pl.pallas_call(
            functools.partial(
                outgoing_kernel, first=first, per_step=per_step, capacity=capacity, clusters=clusters, extra=extra
            ),
            out_shape=out_shape,
            grid_spec=pltpu.PrefetchScalarGridSpec(
                num_scalar_prefetch=4,
                grid=(outgoing // per_step,),
                in_specs=block_specs(per_step, 0) + [whole(x.shape) for x in state],
                out_specs=[whole(x.shape) for x in out_shape],
                scratch_shapes=[pltpu.VMEM((clusters + outgoing, P_SIZE, S), jnp.float32)],
            ),
            compiler_params=params,
            name="outgoing",
        )(order, source, place_sorted, slot, *([link_blocks] * per_step), *state)

    def stay(rounded, acc):
        return pl.pallas_call(
            functools.partial(local_kernel, per_step=per_step, offset=outgoing),
            out_shape=jax.ShapeDtypeStruct(full, jnp.float32),
            grid_spec=pltpu.PrefetchScalarGridSpec(
                num_scalar_prefetch=3,
                grid=((count_links - outgoing) // per_step,),
                in_specs=block_specs(per_step, outgoing) + [whole(full), whole(full)],
                out_specs=whole(full),
            ),
            compiler_params=params,
            name="staying",
        )(order, source, place_sorted, *([link_blocks] * per_step), rounded, acc)

    def exchange(sends):
        return [passed_along(x, axis, step) for x, (axis, step) in zip(sends, MOVES)]

    slot = jnp.zeros((outgoing,), jnp.int32)
    rounded = emission3
    weights = None
    for sweep in range(SWEEPS):
        if sweep == 0:
            acc, *sends = leave(True, slot, emission3, tail)
        else:
            rounded, acc, *sends = leave(False, slot, acc, *arrived, emission3, refl)
        arrived = exchange(sends)
        acc = stay(rounded, acc)
        if sweep == 0:
            items = jnp.concatenate(
                [
                    item_before.at[:, :TAPS].add(-2.0 * rows_here),
                    item_after,
                    item.at[:, :TAPS].add(-1.0 * rows_here),
                ],
                axis=0,
            )
            items, acc = lax.optimization_barrier((items, acc))
            count = items.shape[0]
            block = math.gcd(count, 256)
            weights = pl.pallas_call(
                functools.partial(weights_kernel, tile=16, columns=rows_here),
                out_shape=jax.ShapeDtypeStruct((count, rows_here), jnp.bfloat16),
                grid=(count // block,),
                in_specs=[pl.BlockSpec((block, 2 * TAPS), lambda i: (i, 0))],
                out_specs=pl.BlockSpec((block, rows_here), lambda i: (i, 0)),
                compiler_params=params,
                name="sensor_weights",
            )(items)
            acc, weights, *arrived = lax.optimization_barrier((acc, weights, *arrived))
            slot = jnp.concatenate([x[send_rows : send_rows + capacity, 0] for x in arrived]).astype(jnp.int32)
    rounded, radiosity = pl.pallas_call(
        functools.partial(final_kernel, capacity=capacity, clusters=clusters),
        out_shape=[jax.ShapeDtypeStruct(full, jnp.bfloat16), jax.ShapeDtypeStruct(full, jnp.float32)],
        grid_spec=pltpu.PrefetchScalarGridSpec(
            num_scalar_prefetch=1,
            grid=(1,),
            in_specs=[whole(x.shape) for x in (acc, *arrived, emission3, refl)],
            out_specs=[whole(full), whole(full)],
            scratch_shapes=[pltpu.VMEM(full, jnp.float32)],
        ),
        compiler_params=params,
        name="last",
    )(slot, acc, *arrived, emission3, refl)
    final = rounded.reshape(rows_here, S)
    sensors = item.shape[0]
    beside = jnp.dot(weights[: 2 * sensors], final, preferred_element_type=jnp.float32).astype(jnp.bfloat16)
    to_before = passed_along(beside[:sensors], "gy", -1)
    to_after = passed_along(beside[sensors:], "gy", 1)
    here = jnp.dot(weights[2 * sensors :], final, preferred_element_type=jnp.float32)
    values = here + to_before.astype(jnp.float32) + to_after.astype(jnp.float32)
    return (radiosity.reshape(rows_here, S), values)


def solution(mesh):
    return jax.shard_map(
        per_device,
        mesh=mesh,
        in_specs=(
            P(("gx", "gy"), None),
            P(("gx", "gy")),
            P(("gx", "gy"), None, None),
            P(("gx", "gy")),
            P(("gx", "gy"), None),
            P(("gx", "gy")),
            P(("gx", "gy"), None),
            P(("gx", "gy"), None),
        ),
        out_specs=(P(("gx", "gy"), None), P(("gx", "gy"), None)),
        check_vma=False,
    )
```

```python
import functools
import math

import jax
import jax.numpy as jnp
from jax import lax
from jax.experimental import pallas as pl
from jax.experimental.pallas import tpu as pltpu
from jax.sharding import PartitionSpec as P

P_SIZE = 256
S = 128
SWEEPS = 2
TAPS = 8
MOVES = (("gy", 1), ("gy", -1), ("gx", 1), ("gx", -1))


def passed_along(block, axis, distance):
    devices = range(lax.axis_size(axis))
    route = [(i - distance, i) for i in devices if i - distance in devices]
    return lax.ppermute(block, axis, route)


def per_step_of(*counts):
    common = math.gcd(*counts)
    return max(n for n in range(1, 13) if common % n == 0)


def combine_into(acc_ref, slot_ref, arrived, emission_ref, refl_ref, rounded_ref, rad_ref, capacity, clusters):
    for way in range(4):
        def add(r, carry, way=way):
            slot = slot_ref[way * capacity + r]
            rows = pl.ds(pl.multiple_of(r * P_SIZE, P_SIZE), P_SIZE)
            acc_ref[slot] += arrived[way][rows, :].astype(jnp.float32)
            return carry
        lax.fori_loop(0, capacity, add, 0)

    def finish(c, carry):
        value = emission_ref[c].astype(jnp.float32) + refl_ref[c] * acc_ref[c]
        rounded_ref[c] = value.astype(jnp.bfloat16)
        if rad_ref is not None:
            rad_ref[c] = value
        return carry
    lax.fori_loop(0, clusters, finish, 0)


def add_terms(blocks, source, place, rounded, acc, products, start):
    for g, block in enumerate(blocks):
        products[g] = jnp.dot(block[...], rounded[source[start + g]], preferred_element_type=jnp.float32)
    for g in range(len(blocks)):
        acc[place[start + g]] += products[g]


def outgoing_kernel(order, source, place, slot, *refs, first, per_step, capacity, clusters, extra):
    blocks, refs = refs[:per_step], refs[per_step:]
    if first:
        emission, tail = refs[:2]
        refs = refs[2:]
        rounded = emission
    else:
        acc_in, a0, a1, a2, a3, emission, refl = refs[:7]
        rounded = refs[7]
        refs = refs[8:]
    local, sends, acc, products = refs[0], refs[1:5], refs[5], refs[6]
    step = pl.program_id(0)

    @pl.when(step == 0)
    def _():
        if not first:
            acc[0:clusters] = acc_in[...]
            combine_into(acc, slot, (a0, a1, a2, a3), emission, refl, rounded, None, capacity, clusters)
        acc[...] = jnp.zeros(acc.shape, acc.dtype)

    add_terms(blocks, source, place, rounded, acc, products, step * per_step)

    @pl.when(step == pl.num_programs(0) - 1)
    def _():
        local[...] = acc[0:clusters]
        for way in range(4):
            for r in range(capacity):
                sends[way][r * P_SIZE : (r + 1) * P_SIZE, :] = acc[clusters + way * capacity + r].astype(jnp.bfloat16)
            if first:
                sends[way][capacity * P_SIZE :, :] = tail[way]


def local_kernel(order, source, place, *refs, per_step, offset):
    blocks, refs = refs[:per_step], refs[per_step:]
    rounded, acc_in, acc, products = refs
    step = pl.program_id(0)

    @pl.when(step == 0)
    def _():
        acc[...] = acc_in[...]

    add_terms(blocks, source, place, rounded, acc, products, offset + step * per_step)


def final_kernel(slot, acc_in, a0, a1, a2, a3, emission, refl, rounded, rad, acc, *, capacity, clusters):
    acc[...] = acc_in[...]
    combine_into(acc, slot, (a0, a1, a2, a3), emission, refl, rounded, rad, capacity, clusters)


def weights_kernel(item_ref, out_ref, *, tile, columns):
    def body(t, carry):
        rows = pl.ds(pl.multiple_of(t * tile, tile), tile)
        item = item_ref[rows, :]
        cells = [
            jnp.broadcast_to(item[:, k : k + 1], (tile, 128)).astype(jnp.int32).astype(jnp.int16) for k in range(TAPS)
        ]
        weights = [
            jnp.broadcast_to(item[:, TAPS + k : TAPS + k + 1], (tile, 128)).astype(jnp.bfloat16) for k in range(TAPS)
        ]
        zero = jnp.zeros((tile, 128), jnp.bfloat16)
        lane = lax.broadcasted_iota(jnp.int32, (tile, 128), 1)
        for c in range(columns // 128):
            here = (lane + c * 128).astype(jnp.int16)
            total = jnp.where(cells[0] == here, weights[0], zero)
            for k in range(1, TAPS):
                total = total + jnp.where(cells[k] == here, weights[k], zero)
            out_ref[rows, c * 128 : (c + 1) * 128] = total
        return carry
    lax.fori_loop(0, item_ref.shape[0] // tile, body, 0)


def whole(shape):
    return pl.BlockSpec(shape, lambda *_: (0,) * len(shape))


def block_specs(per_step, offset):
    return [
        pl.BlockSpec((None, P_SIZE, P_SIZE), lambda i, order, *_, g=g: (order[offset + i * per_step + g], 0, 0))
        for g in range(per_step)
    ]


def per_device(
    emission,
    reflectance,
    link_blocks,
    link_source,
    link_target,
    link_slot,
    sensor_cell,
    sensor_weight,
):
    n_cols = lax.axis_size("gy")
    row_here = lax.axis_index("gx")
    col_here = lax.axis_index("gy")
    device_here = row_here * n_cols + col_here
    count_links = link_blocks.shape[0]
    rows_here = emission.shape[0]
    clusters = rows_here // P_SIZE
    capacity = max(2, count_links // 16)
    extra = -(-capacity // 16) * 16
    outgoing = 4 * capacity
    per_step = per_step_of(outgoing, count_links)
    full = (clusters, P_SIZE, S)
    send_rows = capacity * P_SIZE
    products = pltpu.VMEM((per_step, P_SIZE, S), jnp.float32)

    owner = link_target[:, 0]
    owner_row = owner // n_cols
    owner_col = owner % n_cols
    heading = jnp.where(
        owner == device_here,
        0,
        jnp.where(
            owner_row == row_here + 1,
            3,
            jnp.where(owner_row == row_here - 1, 4, jnp.where(owner_col == col_here + 1, 1, 2)),
        ),
    ).astype(jnp.int32)
    number = jnp.arange(count_links, dtype=jnp.int32)
    before = number[None, :] < number[:, None]
    rank = jnp.sum(((heading[:, None] == heading[None, :]) & before).astype(jnp.int32), axis=1)
    local = heading == 0
    ahead = jnp.where(local[:, None], (~local)[None, :] | before, (~local)[None, :] & before)
    position = jnp.sum(ahead.astype(jnp.int32), axis=1)
    place = jnp.where(local, link_slot, clusters + (heading - 1) * capacity + rank)
    turned = position[None, :] == number[:, None]

    def sort(x):
        return jnp.sum(jnp.where(turned, x[None, :], 0), axis=1)

    order, source, place_sorted = sort(number), sort(link_source), sort(place)
    spots = clusters + jnp.arange(outgoing, dtype=jnp.int32)
    sent_slot = jnp.sum(jnp.where(place[None, :] == spots[:, None], (link_slot * (~local))[None, :], 0), axis=1)
    tail = jnp.zeros((4, extra), jnp.bfloat16).at[:, :capacity].set(
        sent_slot.reshape(4, capacity).astype(jnp.bfloat16)
    )
    tail = jnp.broadcast_to(tail[:, :, None], (4, extra, S))

    item = jnp.concatenate([sensor_cell.astype(jnp.float32), sensor_weight], axis=1)
    item_before = passed_along(item, "gy", 1)
    item_after = passed_along(item, "gy", -1)

    emission3 = emission.reshape(full)
    refl = jnp.broadcast_to(reflectance[:, None], (rows_here, S)).reshape(full)
    params = pltpu.CompilerParams(dimension_semantics=("arbitrary",), vmem_limit_bytes=56 * 2**20)

    def leave(first, slot, *state):
        rows = send_rows + (extra if first else 0)
        out_shape = [jax.ShapeDtypeStruct(full, jnp.float32)] + [jax.ShapeDtypeStruct((rows, S), jnp.bfloat16)] * 4
        if not first:
            out_shape = [jax.ShapeDtypeStruct(full, jnp.bfloat16)] + out_shape
        return pl.pallas_call(
            functools.partial(
                outgoing_kernel, first=first, per_step=per_step, capacity=capacity, clusters=clusters, extra=extra
            ),
            out_shape=out_shape,
            grid_spec=pltpu.PrefetchScalarGridSpec(
                num_scalar_prefetch=4,
                grid=(outgoing // per_step,),
                in_specs=block_specs(per_step, 0) + [whole(x.shape) for x in state],
                out_specs=[whole(x.shape) for x in out_shape],
                scratch_shapes=[pltpu.VMEM((clusters + outgoing, P_SIZE, S), jnp.float32), products],
            ),
            compiler_params=params,
            name="outgoing",
        )(order, source, place_sorted, slot, *([link_blocks] * per_step), *state)

    def stay(rounded, acc):
        return pl.pallas_call(
            functools.partial(local_kernel, per_step=per_step, offset=outgoing),
            out_shape=jax.ShapeDtypeStruct(full, jnp.float32),
            grid_spec=pltpu.PrefetchScalarGridSpec(
                num_scalar_prefetch=3,
                grid=((count_links - outgoing) // per_step,),
                in_specs=block_specs(per_step, outgoing) + [whole(full), whole(full)],
                out_specs=whole(full),
                scratch_shapes=[products],
            ),
            compiler_params=params,
            name="staying",
        )(order, source, place_sorted, *([link_blocks] * per_step), rounded, acc)

    def exchange(sends):
        return [passed_along(x, axis, step) for x, (axis, step) in zip(sends, MOVES)]

    def sensor_weights(items):
        count = items.shape[0]
        block = math.gcd(count, 256)
        return pl.pallas_call(
            functools.partial(weights_kernel, tile=16, columns=rows_here),
            out_shape=jax.ShapeDtypeStruct((count, rows_here), jnp.bfloat16),
            grid=(count // block,),
            in_specs=[pl.BlockSpec((block, 2 * TAPS), lambda i: (i, 0))],
            out_specs=pl.BlockSpec((block, rows_here), lambda i: (i, 0)),
            compiler_params=params,
            name="sensor_weights",
        )(items)

    slot = jnp.zeros((outgoing,), jnp.int32)
    rounded = emission3
    weights = []
    for sweep in range(SWEEPS):
        if sweep == 0:
            acc, *sends = leave(True, slot, emission3, tail)
        else:
            rounded, acc, *sends = leave(False, slot, acc, *arrived, emission3, refl)
        arrived = exchange(sends)
        acc = stay(rounded, acc)
        if sweep == 0:
            items = jnp.concatenate(
                [
                    item_before.at[:, :TAPS].add(-2.0 * rows_here),
                    item_after,
                    item.at[:, :TAPS].add(-1.0 * rows_here),
                ],
                axis=0,
            )
        share = items.shape[0] // SWEEPS
        part, acc = lax.optimization_barrier((items[sweep * share : (sweep + 1) * share], acc))
        weights.append(sensor_weights(part))
        acc, weights[sweep], *arrived = lax.optimization_barrier((acc, weights[sweep], *arrived))
        if sweep == 0:
            slot = jnp.concatenate([x[send_rows : send_rows + capacity, 0] for x in arrived]).astype(jnp.int32)
    rounded, radiosity = pl.pallas_call(
        functools.partial(final_kernel, capacity=capacity, clusters=clusters),
        out_shape=[jax.ShapeDtypeStruct(full, jnp.bfloat16), jax.ShapeDtypeStruct(full, jnp.float32)],
        grid_spec=pltpu.PrefetchScalarGridSpec(
            num_scalar_prefetch=1,
            grid=(1,),
            in_specs=[whole(x.shape) for x in (acc, *arrived, emission3, refl)],
            out_specs=[whole(full), whole(full)],
            scratch_shapes=[pltpu.VMEM(full, jnp.float32)],
        ),
        compiler_params=params,
        name="last",
    )(slot, acc, *arrived, emission3, refl)
    final = rounded.reshape(rows_here, S)
    sensors = item.shape[0]
    sums = jnp.concatenate([jnp.dot(w, final, preferred_element_type=jnp.float32) for w in weights], axis=0)
    beside = sums[: 2 * sensors].astype(jnp.bfloat16)
    here = sums[2 * sensors :]
    to_before = passed_along(beside[:sensors], "gy", -1)
    to_after = passed_along(beside[sensors:], "gy", 1)
    values = here + to_before.astype(jnp.float32) + to_after.astype(jnp.float32)
    return (radiosity.reshape(rows_here, S), values)


def solution(mesh):
    return jax.shard_map(
        per_device,
        mesh=mesh,
        in_specs=(
            P(("gx", "gy"), None),
            P(("gx", "gy")),
            P(("gx", "gy"), None, None),
            P(("gx", "gy")),
            P(("gx", "gy"), None),
            P(("gx", "gy")),
            P(("gx", "gy"), None),
            P(("gx", "gy"), None),
        ),
        out_specs=(P(("gx", "gy"), None), P(("gx", "gy"), None)),
        check_vma=False,
    )
```
